32 devices in a mesh: grp: 2 (over y), tile: 4 (over z), coil: 2 (over x), spk: 2 (over core).
Axes of the slice: x: 2, y: 2, z: 4, core: 2. Of those that a mesh axis runs over, the one named last changes fastest.
Arguments:
- coil_maps: float32 [2, 512, 2, 256], P('coil', ('grp', 'tile', 'spk')), parts along dimension 1, may hold values from -6 to 6
- kspace_data: bfloat16 [2, 128, 2, 256], P('coil', ('grp', 'tile', 'spk')), parts along dimension 1, may hold values from -24 to 24
- interp_weights: bfloat16 [128, 6, 256], P(('grp', 'tile', 'spk')), parts along dimension 0, may hold values from 0.099609375 to 1
- sample_bins: int32 [128, 256], P(('grp', 'tile', 'spk')), parts along dimension 0, may hold values from 0 to 65535, as said below
- spoke_count: int32 [16], P(('grp', 'tile', 'spk')), parts along dimension 0, may hold values from 1 to 8, 32 in all
- thresholds: float32 [3], replicated, may hold values from 0.05 to 0.3
Outputs:
- image: float32 [512, 2, 256], P(('grp', 'tile', 'spk')), parts along dimension 0
The draws below stay inside these ranges and needn't reach their ends.
There are 2 independent parts, one for each index of `grp`. The reference program is written for one: setup_inputs(seed, part) draws one part's arguments, and reference() takes and returns one part's arrays. A program takes and returns all parts, laid end to end along the dimension named above; an argument that names none is the same for every part. Nothing has to cross between parts.
Inputs may be any that keep to these rules, and one draw needn't show every extreme that they name: `sample_bins`: sample k of each spoke lies on a straight line through cell (128, 128), at offset k - 128 along the spoke's direction, coordinates taken modulo 256. `spoke_count`: each independent slice has its own 8 counts, and the whole array holds one such block of counts per slice. The 8 counts of each slice sum to 32. In every draw, at least one device of each slice holds 8 live spokes. A device's live spokes are its first ones.
All inputs are finite; a program needn't handle non-finite values.
Results may differ from the reference program's by a relative error of at most 0.0016.
Values may be sent and summed in bfloat16 or wider, within the bound.
A program may use at most 64 MiB of HBM per device.

```python
import math
import jax
import jax.numpy as jnp
import numpy as np
from jax import lax

N = 256
RO = 256
SPK_DEV = 8
LEVELS = 3
ITERS = 4
COILS = 2
BLOCKS = 8
SPOKES = 64


def draw_sample_bins(key, part):
    key_side, key_sign, key_slope = jax.random.split(key, 3)
    middle = N // 2
    side_pick = jax.random.randint(key_side, (SPOKES,), 0, 2)
    sign_pick = jax.random.randint(key_sign, (SPOKES,), 0, 2) * 2 - 1
    slope_val = jax.random.randint(key_slope, (SPOKES,), -middle, middle + 1)
    row_dir = jnp.where(side_pick == 1, sign_pick * middle, slope_val)
    col_dir = jnp.where(side_pick == 1, slope_val, sign_pick * middle)
    offsets = jnp.arange(RO, dtype=jnp.int32) - RO // 2
    row_bins = (middle + offsets[None, :] * row_dir[:, None] * 2 // RO) % N
    col_bins = (middle + offsets[None, :] * col_dir[:, None] * 2 // RO) % N
    return (row_bins * N + col_bins).astype(jnp.int32)


def steps_of(stream_key, dims, cuts, least, high):
    factor_of, own = 1.0, jax.random.fold_in(stream_key, 6)
    for position, parts in cuts:
        steps = jnp.exp(jax.random.uniform(jax.random.fold_in(own, position), (parts,), jnp.float32, least / len(cuts), high / len(cuts)))
        factor_of = factor_of * jnp.repeat(steps, dims[position] // parts).reshape([-1 if axis == position else 1 for axis in range(len(dims))])
    return factor_of


def profile(number_of, total, most, lean):
    portions = [(1 << 20) // math.isqrt(grade ** lean) + 1 for grade in range(2, number_of + 1)]
    surplus, holding = total - most - (number_of - 1), [1] * (number_of - 1)
    while surplus > 0:
        movable = [i for i in range(number_of - 1) if holding[i] < most]
        whole, left = sum([portions[i] for i in movable]), surplus
        for i in movable:
            addition = min(most - holding[i], max(1, left * portions[i] // whole), surplus)
            holding[i] = holding[i] + addition
            surplus = surplus - addition
    return np.array([most] + holding)


def uneven(rng, number_of, total, reach, skew):
    if number_of == 2:
        one = jax.random.randint(rng, (), max(1, total - reach), min(reach, total - 1) + 1)
        return jnp.stack([one, total - one])
    sizes = jnp.asarray(profile(number_of, total, reach, skew), jnp.int32)
    twos = (number_of - 1) // 2
    giver, sink = sizes[1:1 + 2 * twos:2], sizes[2:2 + 2 * twos:2]
    margin = jnp.minimum(giver - 1, reach - sink)
    passed = jax.random.randint(jax.random.fold_in(rng, 1), (twos,), 0, 1 << 20) % (margin + 1)
    sizes = sizes.at[1:1 + 2 * twos:2].set(giver - passed).at[2:2 + 2 * twos:2].set(sink + passed)
    return sizes[jax.random.permutation(jax.random.fold_in(rng, 2), number_of)]


def gaussian(rng, dims, spread, limit, pieces=(), kind=jnp.bfloat16):
    entries = jax.random.normal(rng, dims, jnp.float32) * spread
    if len(pieces) > 0:
        entries = steps_of(rng, dims, pieces, -0.22, 0.18) * entries
    return jnp.clip(entries, min=-limit, max=limit).astype(kind)


def setup_inputs(seed: int = 0, part: int = 0) -> dict:
    splits = jax.random.split(jax.random.key(seed), 7)
    own_keys = jax.random.split(jax.random.fold_in(splits[6], part), 7)
    return {
        "coil_maps": gaussian(own_keys[0], (COILS, N, 2, N), (1.0 / (2.0 * COILS) ** 0.5), 6.0, ((0, 2), (1, 8)), jnp.float32),
        "kspace_data": gaussian(own_keys[1], (COILS, SPOKES, 2, RO), 4.0, 24.0, ((0, 2), (1, 8))),
        "interp_weights": jnp.clip(0.099609375 + 0.9003906 * jax.random.uniform(own_keys[2], (SPOKES, 6, RO), jnp.float32) ** steps_of(own_keys[2], (SPOKES, 6, RO), ((0, 8),), -0.2, 0.2), 0.099609375, 1.0).astype(jnp.bfloat16),
        "sample_bins": draw_sample_bins(jax.random.fold_in(jax.random.fold_in(splits[6], part), 71), part),
        "spoke_count": uneven(own_keys[4], BLOCKS, BLOCKS * SPK_DEV // 2, SPK_DEV, 2).astype(jnp.int32),
        "thresholds": jnp.clip(jax.random.uniform(splits[5], (LEVELS,), jnp.float32, 0.05, 0.3), 0.05, 0.3),
    }


HIGH = lax.Precision.HIGHEST
STEP_SIZE = 0.5
RSQRT2 = 0.7071067811865476

def dft_table(length, direction):
    positions = jnp.arange(length, dtype=jnp.int32)
    phases = positions[:, None] * positions[None, :] % length
    angles = phases.astype(jnp.float32) * jnp.float32(2.0 * math.pi / length)
    norm_scale = 1.0 / math.sqrt(length)
    cosine = jnp.cos(angles) * norm_scale
    sine_tab = jnp.sin(angles) * norm_scale
    top_rows = jnp.stack([cosine, -direction * sine_tab], axis=1)
    bottom = jnp.stack([direction * sine_tab, cosine], axis=1)
    return jnp.stack([top_rows, bottom], axis=0)

def haar_matrix(length, levels):
    haar_mat = jnp.eye(length, dtype=jnp.float32)
    positions = jnp.arange(length, dtype=jnp.int32)
    out_i = positions[:, None]
    in_j = positions[None, :]
    for level_num in range(levels):
        span_len = length >> level_num
        half_len = span_len // 2
        low_hit = (out_i < half_len) & ((in_j == 2 * out_i) | (in_j == 2 * out_i + 1))
        high_pos = out_i - half_len
        high_hit = (out_i >= half_len) & (out_i < span_len) & ((in_j == 2 * high_pos) | (in_j == 2 * high_pos + 1))
        sign_val = jnp.where(in_j == 2 * high_pos + 1, -1.0, 1.0)
        step_mat = jnp.where(low_hit, RSQRT2, jnp.where(high_hit, sign_val * RSQRT2, 0.0))
        step_mat = step_mat + jnp.where((out_i >= span_len) & (in_j == out_i), 1.0, 0.0)
        haar_mat = jnp.dot(step_mat.astype(jnp.float32), haar_mat, precision=HIGH)
    return haar_mat

def haar_labels(length, levels):
    positions = jnp.arange(length, dtype=jnp.int32)
    band_label = jnp.ones((length,), jnp.int32)
    for level_num in range(1, levels + 1):
        band_label = band_label + (positions < length >> level_num).astype(jnp.int32)
    return band_label

def wavelet_shrink(target, thresholds, levels):
    row_count, pair_dim, col_count = target.shape
    block_len = 2 ** levels
    row_haar = haar_matrix(block_len, levels)
    col_haar = haar_matrix(col_count, levels)
    grouped = target.reshape(row_count // block_len, block_len, pair_dim, col_count)
    coeffs = jnp.einsum('ij,gjpc->gipc', row_haar, grouped, precision=HIGH)
    coeffs = jnp.einsum('gipc,kc->gipk', coeffs, col_haar, precision=HIGH)
    band_min = jnp.minimum(haar_labels(block_len, levels)[:, None], haar_labels(col_count, levels)[None, :])
    active = band_min <= levels
    limits = jnp.ones(band_min.shape, jnp.float32)
    for level_num in range(levels):
        limits = jnp.where(band_min == level_num + 1, thresholds[level_num], limits)
    magnitude = jnp.sqrt(coeffs[:, :, 0] ** 2 + coeffs[:, :, 1] ** 2)
    factor = jnp.maximum(magnitude - limits, 0.0) / jnp.maximum(magnitude, limits)
    factor = jnp.where(active, factor, 1.0)
    shrunk = coeffs * factor[:, :, None, :]
    restored = jnp.einsum('gipk,kc->gipc', shrunk, col_haar, precision=HIGH)
    restored = jnp.einsum('ij,gipc->gjpc', row_haar, restored, precision=HIGH)
    return restored.reshape(row_count, pair_dim, col_count)

def complex_mul(left, right):
    real_part = left[:, 0] * right[:, 0] - left[:, 1] * right[:, 1]
    imag_part = left[:, 0] * right[:, 1] + left[:, 1] * right[:, 0]
    return jnp.stack([real_part, imag_part], axis=1)

def conj_mul(left, right):
    real_part = left[:, 0] * right[:, 0] + left[:, 1] * right[:, 1]
    imag_part = left[:, 0] * right[:, 1] - left[:, 1] * right[:, 0]
    return jnp.stack([real_part, imag_part], axis=1)

def reference(coil_maps, kspace_data, interp_weights, sample_bins, spoke_count, thresholds):
    spokes_all = sample_bins.shape[0]
    blocks_all = spoke_count.shape[0]
    per_block = spokes_all // blocks_all
    live_total = spokes_all // 2
    spoke_ids = jnp.arange(spokes_all, dtype=jnp.int32)
    owners = (spoke_ids // per_block).astype(jnp.int32)
    live_mask = (spoke_ids % per_block < spoke_count[owners]).astype(jnp.float32)
    offset = jnp.abs(jnp.arange(RO, dtype=jnp.int32) - RO // 2).astype(jnp.float32)
    density = (offset + 0.5) * (N / (3.0 * RO * live_total))
    row_bins = sample_bins // N
    col_bins = sample_bins % N
    row_taps = [((row_bins + tap_index - 1) % N).astype(jnp.int32) for tap_index in range(3)]
    col_taps = [((col_bins + tap_index - 1) % N).astype(jnp.int32) for tap_index in range(3)]
    weights_f = interp_weights.astype(jnp.float32)
    fwd_table = dft_table(N, 1.0)
    inv_table = dft_table(N, -1.0)

    def coil_gradient(estimate, maps_one, data_one):
        coil_image = complex_mul(maps_one, estimate)
        half_done = jnp.einsum('rpc,pcqv->rqv', coil_image, fwd_table, precision=HIGH)
        kspace = jnp.einsum('rpv,prqu->vqu', half_done, fwd_table, precision=HIGH).astype(jnp.bfloat16)
        kspace = lax.optimization_barrier(kspace).astype(jnp.float32)
        sample_model = jnp.zeros((spokes_all, RO, 2), jnp.float32)
        for col_index in range(3):
            inner_sum = jnp.zeros((spokes_all, RO, 2), jnp.float32)
            for row_index in range(3):
                picked = kspace[col_taps[col_index], :, row_taps[row_index]]
                inner_sum = inner_sum + weights_f[:, row_index, :, None] * picked
            sample_model = sample_model + weights_f[:, 3 + col_index, :, None] * inner_sum
        sample_model = jnp.transpose(sample_model, (0, 2, 1))
        weighted = live_mask[:, None, None] * density[None, None, :] * (sample_model - data_one.astype(jnp.float32))
        gridded = jnp.zeros((N, 2, N), jnp.float32)
        for col_index in range(3):
            smeared = (weights_f[:, 3 + col_index, None, :] * weighted).astype(jnp.bfloat16)
            smeared = lax.optimization_barrier(smeared).astype(jnp.float32)
            smeared_t = jnp.transpose(smeared, (0, 2, 1))
            for row_index in range(3):
                gridded = gridded.at[col_taps[col_index], :, row_taps[row_index]].add(weights_f[:, row_index, :, None] * smeared_t)
        partial_back = jnp.einsum('vpu,puqr->vqr', gridded, inv_table, precision=HIGH)
        coil_back = jnp.einsum('vpr,pvqc->rqc', partial_back, inv_table, precision=HIGH)
        return conj_mul(maps_one, coil_back)
    estimate = jnp.zeros((N, 2, N), jnp.float32)
    for iteration in range(ITERS):
        terms = lax.map(lambda coil_pack: coil_gradient(estimate, coil_pack[0], coil_pack[1]), (coil_maps, kspace_data))
        gradient = lax.optimization_barrier(jnp.sum(terms, axis=0))
        estimate = wavelet_shrink(estimate - STEP_SIZE * gradient, thresholds, LEVELS)
    return estimate
```

```python
import functools
import math

import jax
import jax.numpy as jnp
import numpy as np
from jax import lax
from jax.experimental import pallas as pl
from jax.experimental.pallas import tpu as pltpu
from jax.sharding import PartitionSpec as P

SPK_DEV = 8
LEVELS = 3
ITERS = 4
CORES = 2
CHUNKS = 4
GROUP = 4
STEP_SIZE = 0.5
LANES = 128
F32 = jnp.float32
BF16 = jnp.bfloat16
MESH = pl.DeviceIdType.MESH


def split_np(table):
    high = table.astype(jnp.bfloat16)
    low = (table - high.astype(np.float32)).astype(jnp.bfloat16)
    return high, low


def haar_signs(length, levels):
    mat = np.eye(length)
    for level in range(levels):
        span = length >> level
        half = span // 2
        step = np.eye(length)
        step[:span] = 0.0
        for i in range(half):
            step[i, 2 * i] = step[i, 2 * i + 1] = 1.0
            step[half + i, 2 * i] = 1.0
            step[half + i, 2 * i + 1] = -1.0
        mat = step @ mat
    return mat


def haar_labels(length, levels):
    label = np.ones((length,), np.int32)
    for level in range(1, levels + 1):
        label = label + (np.arange(length) < length >> level)
    return label


def tables(n, levels, chunk):
    phase = np.outer(np.arange(n), np.arange(n)) % n
    angle = phase * (2.0 * np.pi / n)
    cosine = (np.cos(angle) / math.sqrt(n)).astype(np.float32)
    sine = (np.sin(angle) / math.sqrt(n)).astype(np.float32)
    wide = np.concatenate([cosine, sine], axis=1)
    tall = np.concatenate([cosine, sine], axis=0)
    col = haar_signs(n, levels)
    block = 2**levels
    small = haar_signs(block, levels)
    rows = np.kron(np.eye(chunk // block), small)
    col_norm = 1.0 / np.sqrt((col**2).sum(1))
    row_norm = 1.0 / np.sqrt((small**2).sum(1))
    scale = np.tile(row_norm[:, None] * col_norm[None, :], (chunk // block, 1))
    label = np.minimum(haar_labels(block, levels)[:, None], haar_labels(n, levels)[None, :])
    label = np.tile(label, (chunk // block, 1))
    wide_h, wide_l = split_np(wide)
    tall_h, tall_l = split_np(tall)
    as_bf = lambda a: np.ascontiguousarray(a).astype(jnp.bfloat16)
    return (
        wide_h, wide_l, tall_h, tall_l,
        as_bf(col.T), as_bf(col), as_bf(rows), as_bf(rows.T),
        scale.astype(np.float32), label.astype(np.int32),
    )


def split(x):
    high = x.astype(BF16)
    return high, (x - high.astype(F32)).astype(BF16)


def mm(a, b):
    return jnp.dot(a, b, preferred_element_type=F32)


def mm3(a, b):
    return mm(a[0], b[0]) + (mm(a[0], b[1]) + mm(a[1], b[0]))


def kernel(
    dims,
    thr_ref, meta_ref, data_ref, map_ref,
    wide_h, wide_l, tall_h, tall_l, col_t, col_m, row_m, row_t, scale_ref, label_ref,
    out_ref,
    meta_all, data_all, maps, comp, comp_data, row_tab, col_tab, kspace, grid, back_h, back_l,
    half_h, half_l, estimate, grads,
    meta_send, meta_recv, data_send, data_recv, map_send, map_recv, grad_send, grad_recv,
):
    n, tiles, coils, rows, live = dims
    blocks = tiles * CORES
    chunk = n // CHUNKS
    coil, tile, core = lax.axis_index("coil"), lax.axis_index("tile"), lax.axis_index("spk")
    pair, bit = coil // CORES, coil % CORES
    block = tile * CORES + core
    mine = pair * CORES + core

    sends = []
    for d_tile in range(tiles):
        for d_core in range(CORES):
            if d_tile == 0 and d_core == 0:
                continue
            copy = pltpu.make_async_remote_copy(
                src_ref=meta_ref,
                dst_ref=meta_all.at[block],
                send_sem=meta_send.at[d_tile * CORES + d_core],
                recv_sem=meta_recv.at[block],
                device_id={"tile": (tile + d_tile) % tiles, "spk": (core + d_core) % CORES},
                device_id_type=MESH,
            )
            copy.start()
            sends.append(copy)
    for src, dst, s_sem, r_sem in (
        (data_ref, data_all.at[block], data_send, data_recv),
        (map_ref, maps.at[:, block], map_send, map_recv),
    ):
        for d_bit in range(CORES):
            for d_tile in range(tiles):
                copy = pltpu.make_async_remote_copy(
                    src_ref=src,
                    dst_ref=dst,
                    send_sem=s_sem.at[d_bit * tiles + d_tile],
                    recv_sem=r_sem.at[block],
                    device_id={
                        "coil": pair * CORES + (bit + d_bit) % CORES,
                        "tile": (tile + d_tile) % tiles,
                        "spk": bit,
                    },
                    device_id_type=MESH,
                )
                if d_bit == 0 and d_tile == 0:
                    local_copy = pltpu.make_async_copy(src, dst, r_sem.at[block])

                    @pl.when(core == bit)
                    def _(local_copy=local_copy):
                        local_copy.start()

                    @pl.when(core != bit)
                    def _(copy=copy):
                        copy.start()
                        copy.wait_send()
                else:
                    copy.start()
                    sends.append(copy)

    meta_all[block] = meta_ref[...]
    for d_block in range(1, blocks):
        other = (block + d_block) % blocks
        pltpu.make_async_copy(meta_all.at[other], meta_all.at[other], meta_recv.at[other]).wait()

    slots = blocks * SPK_DEV * 2
    packed = meta_all[...].reshape(slots, meta_ref.shape[1])
    up = lax.broadcasted_iota(jnp.int32, (slots, slots), 0) // 2
    across = lax.broadcasted_iota(jnp.int32, (slots, slots), 1) // 2
    parity = lax.broadcasted_iota(jnp.int32, (slots, LANES), 0) % 2
    flag = jnp.where((packed[:, :LANES].astype(F32) >= 0.0) & (parity == 0), 1.0 / LANES, 0.0)
    flags = lax.dot_general(
        jnp.ones((LANES, LANES), BF16), flag.astype(BF16), (((1,), (1,)), ((), ())),
        preferred_element_type=F32,
    ).astype(BF16)
    rank = mm(flags, jnp.where(up < across, 1.0, 0.0).astype(BF16))
    alive = mm(flags, jnp.where(up == across, 1.0, 0.0).astype(BF16))
    place = lax.broadcasted_iota(jnp.int32, (LANES, slots), 0)
    which = lax.broadcasted_iota(jnp.int32, (LANES, slots), 1) % 2
    hit = (alive > 0.5) & (rank.astype(jnp.int32) == place)
    pick = [jnp.where(hit & (which == h), 1.0, 0.0).astype(BF16) for h in range(2)]
    for h in range(2):
        comp[h] = mm(pick[h], packed)

    cells = lax.broadcasted_iota(jnp.int32, (n, n), 0)

    def build(i, carry):
        def table(centre, weights):
            gap = (cells - centre.astype(jnp.int32) + 1) & (n - 1)
            return jnp.where(
                gap == 0, weights[0], jnp.where(gap == 1, weights[1], jnp.where(gap == 2, weights[2], 0.0))
            ).astype(BF16)

        def part(h, j):
            return comp[h, pl.ds(i, 1), j * n : (j + 1) * n]

        row_tab[i] = table(part(0, 0), (part(0, 2), part(0, 3), part(1, 0)))
        col_tab[i] = table(part(0, 1), (part(1, 1), part(1, 2), part(1, 3)))
        return carry

    lax.fori_loop(0, live, build, 0)

    for b in range(blocks):
        pltpu.make_async_copy(data_all.at[b], data_all.at[b], data_recv.at[b]).wait()
    samples = data_all[...].reshape(slots, n)
    for h in range(2):
        comp_data[h] = mm(pick[h], samples)

    offset = jnp.abs(lax.broadcasted_iota(jnp.int32, (1, n), 1) - n // 2).astype(F32)
    density = (offset + 0.5) * (n / (3.0 * n * live))
    wide = (wide_h[...], wide_l[...])
    tall = (tall_h[...], tall_l[...])

    for it in range(ITERS):
        slot = it % 2
        grid[...] = jnp.zeros_like(grid)

        def spokes(step, carry, it=it):
            total = None
            for g in range(GROUP):
                i = step * GROUP + g
                real = -comp_data[0, pl.ds(i, 1), :]
                imag = -comp_data[1, pl.ds(i, 1), :]
                col = col_tab[i]
                if it > 0:
                    inner = mm(kspace[...], col)
                    row = row_tab[i].astype(F32)
                    real = real + jnp.sum(inner[:n] * row, axis=0, keepdims=True)
                    imag = imag + jnp.sum(inner[n:] * row, axis=0, keepdims=True)
                real, imag = density * real, density * imag
                wide_col = col.astype(F32)
                smeared = jnp.concatenate(
                    [(wide_col * real).astype(BF16), (wide_col * imag).astype(BF16)], axis=0
                )
                added = lax.dot_general(
                    row_tab[i], smeared, (((1,), (1,)), ((), ())), preferred_element_type=F32
                )
                total = added if total is None else total + added
            grid[...] += total
            return carry

        lax.fori_loop(0, live // GROUP, spokes, 0)

        turned = mm3(tall, split(grid[...]))
        for p, value in enumerate(
            (turned[:n, :n] - turned[n:, n:], turned[:n, n:] + turned[n:, :n])
        ):
            back_h[p], back_l[p] = split(value)
        if it == 0:
            for b in range(blocks):
                pltpu.make_async_copy(maps.at[:, b], maps.at[:, b], map_recv.at[b]).wait()

        def sens(q):
            whole = maps.at[:, pl.ds(q * (blocks // CHUNKS), blocks // CHUNKS)][...]
            whole = whole.reshape(2, chunk, n)
            return whole[0], whole[1]

        copies = []
        for q in range(CHUNKS):
            rs = slice(q * chunk, (q + 1) * chunk)
            b_h = back_h[:, rs, :].reshape(2 * chunk, n)
            b_l = back_l[:, rs, :].reshape(2 * chunk, n)
            image = mm3((b_h, b_l), wide)
            d_r = image[:chunk, :n] - image[chunk:, n:]
            d_i = image[:chunk, n:] + image[chunk:, :n]
            m_r, m_i = sens(q)
            grads[slot, q, mine, 0] = m_r * d_r + m_i * d_i
            grads[slot, q, mine, 1] = m_r * d_i - m_i * d_r
            for d in range(1, coils):
                d_pair, d_core = d // CORES, d % CORES
                copy = pltpu.make_async_remote_copy(
                    src_ref=grads.at[slot, q, mine],
                    dst_ref=grads.at[slot, q, mine],
                    send_sem=grad_send.at[slot, q, d],
                    recv_sem=grad_recv.at[slot, q, mine],
                    device_id={
                        "coil": (coil + d_pair * CORES) % coils,
                        "spk": (core + d_core) % CORES,
                    },
                    device_id_type=MESH,
                )
                copy.start()
                copies.append(copy)

        limits = jnp.ones((chunk, n), F32)
        label = label_ref[...]
        for level in range(LEVELS):
            limits = jnp.where(label == level + 1, thr_ref[level], limits)
        active = label <= LEVELS
        scale = scale_ref[...]
        for q in range(CHUNKS):
            for d in range(1, coils):
                d_pair, d_core = d // CORES, d % CORES
                other = (coil + d_pair * CORES) % coils // CORES * CORES + (core + d_core) % CORES
                pltpu.make_async_copy(
                    grads.at[slot, q, other], grads.at[slot, q, other], grad_recv.at[slot, q, other]
                ).wait()
            summed = grads[slot, q, 0]
            for c in range(1, coils):
                summed = summed + grads[slot, q, c]
            rs = slice(q * chunk, (q + 1) * chunk)
            target = -STEP_SIZE * summed
            if it > 0:
                target = estimate[:, rs, :] + target
            t_h, t_l = split(target.reshape(2 * chunk, n))
            along = mm(t_h, col_t[...]) + mm(t_l, col_t[...])
            side = split(jnp.concatenate([along[:chunk], along[chunk:]], axis=1))
            coeffs = mm(row_m[...], side[0]) + mm(row_m[...], side[1])
            c_r, c_i = coeffs[:, :n] * scale, coeffs[:, n:] * scale
            size = jnp.sqrt(c_r * c_r + c_i * c_i)
            factor = jnp.maximum(size - limits, 0.0) / jnp.maximum(size, limits)
            factor = jnp.where(active, factor, 1.0) * scale
            side = split(jnp.concatenate([c_r * factor, c_i * factor], axis=1))
            along = mm(row_t[...], side[0]) + mm(row_t[...], side[1])
            t_h, t_l = split(jnp.concatenate([along[:, :n], along[:, n:]], axis=0))
            fresh = mm(t_h, col_m[...]) + mm(t_l, col_m[...])
            e_r, e_i = fresh[:chunk], fresh[chunk:]
            estimate[0, rs, :] = e_r
            estimate[1, rs, :] = e_i
            if it < ITERS - 1:
                m_r, m_i = sens(q)
                seen = split(
                    jnp.concatenate([m_r * e_r - m_i * e_i, m_r * e_i + m_i * e_r], axis=0)
                )
                w = mm3(seen, wide)
                half = jnp.concatenate(
                    [w[:chunk, :n] + w[chunk:, n:], w[chunk:, :n] - w[:chunk, n:]], axis=1
                )
                half_h[rs, :], half_l[rs, :] = split(half)
        for copy in copies:
            copy.wait_send()
        if it < ITERS - 1:
            v = mm3(tall, (half_h[...], half_l[...]))
            kspace[:n, :] = (v[:n, :n] + v[n:, n:]).astype(BF16)
            kspace[n:, :] = (v[:n, n:] - v[n:, :n]).astype(BF16)

    out_ref[...] = estimate[:, pl.ds(pl.multiple_of(block * rows, rows), rows), :]
    for copy in sends:
        copy.wait_send()


def local(coil_maps, kspace_data, interp_weights, sample_bins, spoke_count, thresholds):
    tiles, coils = lax.axis_size("tile"), lax.axis_size("coil")
    blocks = tiles * CORES
    rows, n = coil_maps.shape[1], coil_maps.shape[3]
    live = blocks * SPK_DEV // 2
    chunk = n // CHUNKS
    slot_live = jnp.arange(SPK_DEV, dtype=jnp.int32)[:, None] < spoke_count[0]
    row = jnp.where(slot_live, sample_bins // n, -1).astype(BF16)
    col = (sample_bins % n).astype(BF16)
    meta = jnp.concatenate([row[:, None], col[:, None], interp_weights], axis=1)
    meta = meta.reshape(SPK_DEV * 2, 4 * n)
    data = kspace_data[0].reshape(SPK_DEV * 2, n)
    maps = jnp.transpose(coil_maps[0], (1, 0, 2))
    consts = tables(n, LEVELS, chunk)
    vmem = pl.BlockSpec(memory_space=pltpu.VMEM)
    slots = blocks * SPK_DEV * 2
    dma = pltpu.SemaphoreType.DMA
    out = pl.pallas_call(
        functools.partial(kernel, (n, tiles, coils, rows, live)),
        out_shape=jax.ShapeDtypeStruct((2, rows, n), F32),
        in_specs=[pl.BlockSpec(memory_space=pltpu.SMEM)] + [vmem] * (3 + len(consts)),
        out_specs=vmem,
        scratch_shapes=[
            pltpu.VMEM((blocks, SPK_DEV * 2, 4 * n), BF16),
            pltpu.VMEM((blocks, SPK_DEV * 2, n), BF16),
            pltpu.VMEM((2, blocks, rows, n), F32),
            pltpu.VMEM((2, LANES, 4 * n), F32),
            pltpu.VMEM((2, LANES, n), F32),
            pltpu.VMEM((live, n, n), BF16),
            pltpu.VMEM((live, n, n), BF16),
            pltpu.VMEM((2 * n, n), BF16),
            pltpu.VMEM((n, 2 * n), F32),
            pltpu.VMEM((2, n, n), BF16),
            pltpu.VMEM((2, n, n), BF16),
            pltpu.VMEM((n, 2 * n), BF16),
            pltpu.VMEM((n, 2 * n), BF16),
            pltpu.VMEM((2, n, n), F32),
            pltpu.VMEM((2, CHUNKS, coils, 2, chunk, n), F32),
            dma((blocks,)), dma((blocks,)), dma((blocks,)), dma((blocks,)),
            dma((blocks,)), dma((blocks,)),
            dma((2, CHUNKS, coils)), dma((2, CHUNKS, coils)),
        ],
        compiler_params=pltpu.CompilerParams(
            has_side_effects=True, vmem_limit_bytes=60 * 1024 * 1024
        ),
    )(thresholds, meta, data, maps, *consts)
    return jnp.transpose(out, (1, 0, 2))


def solution(mesh):
    placed = (
        P("coil", ("grp", "tile", "spk"), None, None),
        P("coil", ("grp", "tile", "spk"), None, None),
        P(("grp", "tile", "spk"), None, None),
        P(("grp", "tile", "spk"), None),
        P(("grp", "tile", "spk")),
        P(),
    )
    return jax.shard_map(
        local,
        mesh=mesh,
        in_specs=placed,
        out_specs=P(("grp", "tile", "spk"), None, None),
        check_vma=False,
    )
```

```python
import functools
import math

import jax
import jax.numpy as jnp
import numpy as np
from jax import lax
from jax.experimental import pallas as pl
from jax.experimental.pallas import tpu as pltpu
from jax.sharding import PartitionSpec as P

SPK_DEV = 8
LEVELS = 3
ITERS = 4
CORES = 2
CHUNKS = 2
GROUP = 4
STEP_SIZE = 0.5
LANES = 128
F32 = jnp.float32
BF16 = jnp.bfloat16
MESH = pl.DeviceIdType.MESH


def split_np(table):
    high = table.astype(jnp.bfloat16)
    low = (table - high.astype(np.float32)).astype(jnp.bfloat16)
    return high, low


def haar_signs(length, levels):
    mat = np.eye(length)
    for level in range(levels):
        span = length >> level
        half = span // 2
        step = np.eye(length)
        step[:span] = 0.0
        for i in range(half):
            step[i, 2 * i] = step[i, 2 * i + 1] = 1.0
            step[half + i, 2 * i] = 1.0
            step[half + i, 2 * i + 1] = -1.0
        mat = step @ mat
    return mat


def haar_labels(length, levels):
    label = np.ones((length,), np.int32)
    for level in range(1, levels + 1):
        label = label + (np.arange(length) < length >> level)
    return label


def tables(n, levels, chunk):
    phase = np.outer(np.arange(n), np.arange(n)) % n
    angle = phase * (2.0 * np.pi / n)
    cosine = (np.cos(angle) / math.sqrt(n)).astype(np.float32)
    sine = (np.sin(angle) / math.sqrt(n)).astype(np.float32)
    wide = np.concatenate([cosine, sine], axis=1)
    tall = np.concatenate([cosine, sine], axis=0)
    col = haar_signs(n, levels)
    block = 2**levels
    small = haar_signs(block, levels)
    rows = np.kron(np.eye(chunk // block), small)
    col_norm = 1.0 / np.sqrt((col**2).sum(1))
    row_norm = 1.0 / np.sqrt((small**2).sum(1))
    scale = np.tile(row_norm[:, None] * col_norm[None, :], (chunk // block, 1))
    label = np.minimum(haar_labels(block, levels)[:, None], haar_labels(n, levels)[None, :])
    label = np.tile(label, (chunk // block, 1))
    wide_h, wide_l = split_np(wide)
    tall_h, tall_l = split_np(tall)
    as_bf = lambda a: np.ascontiguousarray(a).astype(jnp.bfloat16)
    return (
        wide_h, wide_l, tall_h, tall_l,
        as_bf(col.T), as_bf(col), as_bf(rows), as_bf(rows.T),
        np.ascontiguousarray(scale.T).astype(np.float32), np.ascontiguousarray(label.T).astype(np.int32),
    )


def split(x):
    high = x.astype(BF16)
    return high, (x - high.astype(F32)).astype(BF16)


def mm(a, b):
    return jnp.dot(a, b, preferred_element_type=F32)


def mm3(a, b):
    return mm(a[0], b[0]) + (mm(a[0], b[1]) + mm(a[1], b[0]))


def kernel(
    dims,
    thr_ref, meta_ref, data_ref, map_ref,
    wide_h, wide_l, tall_h, tall_l, col_t, col_m, row_m, row_t, scale_ref, label_ref,
    out_ref,
    meta_all, data_all, maps, comp, comp_data, row_tab, col_tab, kspace, grid, back_h, back_l,
    half_h, half_l, estimate, grads, sens,
    meta_send, meta_recv, data_send, data_recv, map_send, map_recv, grad_send, grad_recv,
):
    n, tiles, coils, rows, live = dims
    blocks = tiles * CORES
    chunk = n // CHUNKS
    coil, tile, core = lax.axis_index("coil"), lax.axis_index("tile"), lax.axis_index("spk")
    pair, bit = coil // CORES, coil % CORES
    block = tile * CORES + core
    mine = pair * CORES + core

    barrier = pltpu.get_barrier_semaphore()
    peers = [
        (d_bit, d_tile, d_core)
        for d_bit in range(CORES)
        for d_tile in range(tiles)
        for d_core in range(CORES)
        if d_bit + d_tile + d_core > 0
    ]
    for d_bit, d_tile, d_core in peers:
        pl.semaphore_signal(
            barrier,
            inc=1,
            device_id={
                "coil": pair * CORES + (bit + d_bit) % CORES,
                "tile": (tile + d_tile) % tiles,
                "spk": (core + d_core) % CORES,
            },
            device_id_type=MESH,
        )
    for d in range(CORES, coils):
        pl.semaphore_signal(
            barrier,
            inc=1,
            device_id={
                "coil": (coil + d // CORES * CORES) % coils,
                "spk": (core + d % CORES) % CORES,
            },
            device_id_type=MESH,
        )
    pl.semaphore_wait(barrier, len(peers) + coils - CORES)

    sends = []
    for d_tile in range(tiles):
        for d_core in range(CORES):
            if d_tile == 0 and d_core == 0:
                continue
            copy = pltpu.make_async_remote_copy(
                src_ref=meta_ref,
                dst_ref=meta_all.at[block],
                send_sem=meta_send.at[d_tile * CORES + d_core],
                recv_sem=meta_recv.at[block],
                device_id={"tile": (tile + d_tile) % tiles, "spk": (core + d_core) % CORES},
                device_id_type=MESH,
            )
            copy.start()
            sends.append(copy)
    across_core = []
    for src, dst, s_sem, r_sem in (
        (data_ref, data_all.at[block], data_send, data_recv),
        (map_ref, maps.at[:, block], map_send, map_recv),
    ):
        for d_bit in range(CORES):
            for d_tile in range(tiles):
                copy = pltpu.make_async_remote_copy(
                    src_ref=src,
                    dst_ref=dst,
                    send_sem=s_sem.at[d_bit * tiles + d_tile],
                    recv_sem=r_sem.at[block],
                    device_id={
                        "coil": pair * CORES + (bit + d_bit) % CORES,
                        "tile": (tile + d_tile) % tiles,
                        "spk": bit,
                    },
                    device_id_type=MESH,
                )
                if d_bit == 0 and d_tile == 0:
                    local_copy = pltpu.make_async_copy(src, dst, r_sem.at[block])

                    @pl.when(core == bit)
                    def _(local_copy=local_copy):
                        local_copy.start()

                    @pl.when(core != bit)
                    def _(copy=copy):
                        copy.start()

                    across_core.append(copy)
                else:
                    copy.start()
                    sends.append(copy)

    meta_all[block] = meta_ref[...]
    for d_block in range(1, blocks):
        other = (block + d_block) % blocks
        pltpu.make_async_copy(meta_all.at[other], meta_all.at[other], meta_recv.at[other]).wait()

    slots = blocks * SPK_DEV * 2
    packed = meta_all[...].reshape(slots, meta_ref.shape[1])
    up = lax.broadcasted_iota(jnp.int32, (slots, slots), 0) // 2
    across = lax.broadcasted_iota(jnp.int32, (slots, slots), 1) // 2
    parity = lax.broadcasted_iota(jnp.int32, (slots, LANES), 0) % 2
    flag = jnp.where((packed[:, :LANES].astype(F32) >= 0.0) & (parity == 0), 1.0 / LANES, 0.0)
    flags = lax.dot_general(
        jnp.ones((LANES, LANES), BF16), flag.astype(BF16), (((1,), (1,)), ((), ())),
        preferred_element_type=F32,
    ).astype(BF16)
    rank = mm(flags, jnp.where(up < across, 1.0, 0.0).astype(BF16))
    alive = mm(flags, jnp.where(up == across, 1.0, 0.0).astype(BF16))
    place = lax.broadcasted_iota(jnp.int32, (LANES, slots), 0)
    which = lax.broadcasted_iota(jnp.int32, (LANES, slots), 1) % 2
    hit = (alive > 0.5) & (rank.astype(jnp.int32) == place)
    pick = [jnp.where(hit & (which == h), 1.0, 0.0).astype(BF16) for h in range(2)]
    for h in range(2):
        comp[h] = mm(pick[h], packed)

    cells = lax.broadcasted_iota(jnp.int32, (n, n), 0)

    def build(i, carry):
        def table(centre, weights):
            gap = (cells - centre.astype(jnp.int32) + 1) & (n - 1)
            return jnp.where(
                gap == 0, weights[0], jnp.where(gap == 1, weights[1], jnp.where(gap == 2, weights[2], 0.0))
            ).astype(BF16)

        def part(h, j):
            return comp[h, pl.ds(i, 1), j * n : (j + 1) * n]

        row_tab[i] = table(part(0, 0), (part(0, 2), part(0, 3), part(1, 0)))
        col_tab[i] = table(part(0, 1), (part(1, 1), part(1, 2), part(1, 3)))
        return carry

    lax.fori_loop(0, live, build, 0)

    for b in range(blocks):
        pltpu.make_async_copy(data_all.at[b], data_all.at[b], data_recv.at[b]).wait()
    samples = data_all[...].reshape(slots, n)
    for h in range(2):
        comp_data[h] = mm(pick[h], samples)

    offset = jnp.abs(lax.broadcasted_iota(jnp.int32, (1, n), 1) - n // 2).astype(F32)
    density = (offset + 0.5) * (n / (3.0 * n * live))
    wide = (wide_h[...], wide_l[...])
    tall = (tall_h[...], tall_l[...])

    for it in range(ITERS):
        slot = it % 2
        grid[...] = jnp.zeros_like(grid)

        def spokes(step, carry, it=it):
            total = None
            for g in range(GROUP):
                i = step * GROUP + g
                real = -comp_data[0, pl.ds(i, 1), :]
                imag = -comp_data[1, pl.ds(i, 1), :]
                col = col_tab[i].astype(F32)
                if it > 0:
                    inner = mm(kspace[...], row_tab[i])
                    real = real + jnp.sum(inner[:n] * col, axis=0, keepdims=True)
                    imag = imag + jnp.sum(inner[n:] * col, axis=0, keepdims=True)
                real, imag = density * real, density * imag
                smeared = jnp.concatenate(
                    [(col * real).astype(BF16), (col * imag).astype(BF16)], axis=0
                )
                added = lax.dot_general(
                    smeared, row_tab[i], (((1,), (1,)), ((), ())), preferred_element_type=F32
                )
                total = added if total is None else total + added
            grid[...] += total
            return carry

        lax.fori_loop(0, live // GROUP, spokes, 0)

        turned = mm3(split(grid[...]), wide)
        for p, value in enumerate(
            (turned[:n, :n] - turned[n:, n:], turned[:n, n:] + turned[n:, :n])
        ):
            back_h[p], back_l[p] = split(value)
        if it == 0:
            for b in range(blocks):
                pltpu.make_async_copy(maps.at[:, b], maps.at[:, b], map_recv.at[b]).wait()

            per_chunk = blocks // CHUNKS
            for p in range(2):
                for q in range(CHUNKS):
                    part = maps[p, q * per_chunk : (q + 1) * per_chunk].reshape(chunk, n)
                    sens[p, q] = part.T

        copies = []
        for q in range(CHUNKS):
            rs = slice(q * chunk, (q + 1) * chunk)
            b_h = jnp.concatenate([back_h[0, :, rs], back_h[1, :, rs]], axis=1)
            b_l = jnp.concatenate([back_l[0, :, rs], back_l[1, :, rs]], axis=1)
            image = mm3(tall, (b_h, b_l))
            d_r = image[:n, :chunk] - image[n:, chunk:]
            d_i = image[:n, chunk:] + image[n:, :chunk]
            m_r, m_i = sens[0, q], sens[1, q]
            grads[slot, q, mine, 0] = m_r * d_r + m_i * d_i
            grads[slot, q, mine, 1] = m_r * d_i - m_i * d_r
            for d in range(1, coils):
                d_pair, d_core = d // CORES, d % CORES
                copy = pltpu.make_async_remote_copy(
                    src_ref=grads.at[slot, q, mine],
                    dst_ref=grads.at[slot, q, mine],
                    send_sem=grad_send.at[slot, q, d],
                    recv_sem=grad_recv.at[slot, q, mine],
                    device_id={
                        "coil": (coil + d_pair * CORES) % coils,
                        "spk": (core + d_core) % CORES,
                    },
                    device_id_type=MESH,
                )
                copy.start()
                copies.append(copy)

        limits = jnp.ones((n, chunk), F32)
        label = label_ref[...]
        for level in range(LEVELS):
            limits = jnp.where(label == level + 1, thr_ref[level], limits)
        active = label <= LEVELS
        scale = scale_ref[...]
        for q in range(CHUNKS):
            for d in range(1, coils):
                d_pair, d_core = d // CORES, d % CORES
                other = (coil + d_pair * CORES) % coils // CORES * CORES + (core + d_core) % CORES
                pltpu.make_async_copy(
                    grads.at[slot, q, other], grads.at[slot, q, other], grad_recv.at[slot, q, other]
                ).wait()
            summed = grads[slot, q, 0]
            for c in range(1, coils):
                summed = summed + grads[slot, q, c]
            rs = slice(q * chunk, (q + 1) * chunk)
            target = -STEP_SIZE * summed
            if it > 0:
                target = estimate[:, q] + target
            side = split(jnp.concatenate([target[0], target[1]], axis=1))
            along = mm(col_m[...], side[0]) + mm(col_m[...], side[1])
            side = split(jnp.concatenate([along[:, :chunk], along[:, chunk:]], axis=0))
            coeffs = mm(side[0], row_t[...]) + mm(side[1], row_t[...])
            c_r, c_i = coeffs[:n] * scale, coeffs[n:] * scale
            size = jnp.sqrt(c_r * c_r + c_i * c_i)
            factor = jnp.maximum(size - limits, 0.0) / jnp.maximum(size, limits)
            factor = jnp.where(active, factor, 1.0) * scale
            side = split(jnp.concatenate([c_r * factor, c_i * factor], axis=0))
            along = mm(side[0], row_m[...]) + mm(side[1], row_m[...])
            side = split(jnp.concatenate([along[:n], along[n:]], axis=1))
            fresh = mm(col_t[...], side[0]) + mm(col_t[...], side[1])
            e_r, e_i = fresh[:, :chunk], fresh[:, chunk:]
            estimate[0, q] = e_r
            estimate[1, q] = e_i
            if it < ITERS - 1:
                m_r, m_i = sens[0, q], sens[1, q]
                seen = split(
                    jnp.concatenate([m_r * e_r - m_i * e_i, m_r * e_i + m_i * e_r], axis=1)
                )
                w = mm3(tall, seen)
                half = jnp.concatenate(
                    [w[:n, :chunk] + w[n:, chunk:], w[:n, chunk:] - w[n:, :chunk]], axis=0
                )
                half_h[:, rs], half_l[:, rs] = split(half)
            else:
                per_chunk = blocks // CHUNKS
                maps[0, q * per_chunk : (q + 1) * per_chunk] = e_r.T.reshape(per_chunk, rows, n)
                maps[1, q * per_chunk : (q + 1) * per_chunk] = e_i.T.reshape(per_chunk, rows, n)
        for copy in copies:
            copy.wait_send()
        if it < ITERS - 1:
            v = mm3((half_h[...], half_l[...]), wide)
            kspace[:n, :] = (v[:n, :n] + v[n:, n:]).astype(BF16)
            kspace[n:, :] = (v[n:, :n] - v[:n, n:]).astype(BF16)

    out_ref[...] = maps[:, block]

    @pl.when(core != bit)
    def _():
        for copy in across_core:
            copy.wait_send()

    for copy in sends:
        copy.wait_send()


def local(coil_maps, kspace_data, interp_weights, sample_bins, spoke_count, thresholds):
    tiles, coils = lax.axis_size("tile"), lax.axis_size("coil")
    blocks = tiles * CORES
    rows, n = coil_maps.shape[1], coil_maps.shape[3]
    live = blocks * SPK_DEV // 2
    chunk = n // CHUNKS
    slot_live = jnp.arange(SPK_DEV, dtype=jnp.int32)[:, None] < spoke_count[0]
    row = jnp.where(slot_live, sample_bins // n, -1).astype(BF16)
    col = (sample_bins % n).astype(BF16)
    meta = jnp.concatenate([row[:, None], col[:, None], interp_weights], axis=1)
    meta = meta.reshape(SPK_DEV * 2, 4 * n)
    data = kspace_data[0].reshape(SPK_DEV * 2, n)
    maps = jnp.transpose(coil_maps[0], (1, 0, 2))
    consts = tables(n, LEVELS, chunk)
    vmem = pl.BlockSpec(memory_space=pltpu.VMEM)
    slots = blocks * SPK_DEV * 2
    dma = pltpu.SemaphoreType.DMA
    out = pl.pallas_call(
        functools.partial(kernel, (n, tiles, coils, rows, live)),
        out_shape=jax.ShapeDtypeStruct((2, rows, n), F32),
        in_specs=[pl.BlockSpec(memory_space=pltpu.SMEM)] + [vmem] * (3 + len(consts)),
        out_specs=vmem,
        scratch_shapes=[
            pltpu.VMEM((blocks, SPK_DEV * 2, 4 * n), BF16),
            pltpu.VMEM((blocks, SPK_DEV * 2, n), BF16),
            pltpu.VMEM((2, blocks, rows, n), F32),
            pltpu.VMEM((2, LANES, 4 * n), F32),
            pltpu.VMEM((2, LANES, n), F32),
            pltpu.VMEM((live, n, n), BF16),
            pltpu.VMEM((live, n, n), BF16),
            pltpu.VMEM((2 * n, n), BF16),
            pltpu.VMEM((2 * n, n), F32),
            pltpu.VMEM((2, n, n), BF16),
            pltpu.VMEM((2, n, n), BF16),
            pltpu.VMEM((2 * n, n), BF16),
            pltpu.VMEM((2 * n, n), BF16),
            pltpu.VMEM((2, CHUNKS, n, chunk), F32),
            pltpu.VMEM((2, CHUNKS, coils, 2, n, chunk), F32),
            pltpu.VMEM((2, CHUNKS, n, chunk), F32),
            dma((blocks,)), dma((blocks,)), dma((blocks,)), dma((blocks,)),
            dma((blocks,)), dma((blocks,)),
            dma((2, CHUNKS, coils)), dma((2, CHUNKS, coils)),
        ],
        compiler_params=pltpu.CompilerParams(
            has_side_effects=True, collective_id=0, vmem_limit_bytes=60 * 1024 * 1024
        ),
    )(thresholds, meta, data, maps, *consts)
    return jnp.transpose(out, (1, 0, 2))


def solution(mesh):
    placed = (
        P("coil", ("grp", "tile", "spk"), None, None),
        P("coil", ("grp", "tile", "spk"), None, None),
        P(("grp", "tile", "spk"), None, None),
        P(("grp", "tile", "spk"), None),
        P(("grp", "tile", "spk")),
        P(),
    )
    return jax.shard_map(
        local,
        mesh=mesh,
        in_specs=placed,
        out_specs=P(("grp", "tile", "spk"), None, None),
        check_vma=False,
    )
```
